32 devices in a mesh: ifg: 4 (over y, x), pix: 8 (over z, core).
Axes of the slice: x: 2, y: 2, z: 4, core: 2. Of those that a mesh axis runs over, the one named last changes fastest.
Arguments:
- phase: bfloat16 [1200, 12288], P('ifg', 'pix'), may hold values from -8 to 8
- incidence: int32 [2304, 1200], P('ifg'), may hold values from -1 to 1, as said below
- triplet_weight: float32 [2304], P('ifg'), may hold values from 0.3 to 3
- date_pairs: int32 [1200, 2], P('ifg'), may hold values from 0 to 249, as said below
Outputs:
- residual: float32 [2304, 12288], P('ifg', 'pix')
- relative: float32 [12288], P('pix')
- corrected: float32 [1200, 12288], P('ifg', 'pix')
The draws below stay inside these ranges and needn't reach their ends.
Inputs may be any that keep to these rules, and one draw needn't show every extreme that they name: `incidence`: each row is a closure triplet of three dates a < b < c whose three interferograms all appear in date_pairs: +1 on (a, b) and on (b, c), -1 on (a, c), zeros elsewhere. No two rows are equal. `date_pairs`: interferograms are listed by first date, then by second date; the second date is 1 to 5 dates after the first, and no pair appears twice.
All inputs are finite; a program needn't handle non-finite values.
Results may differ from the reference program's by a relative error of at most 0.013.
Values may be sent and summed in bfloat16 or wider, within the bound.
No kernel may reach another device: no remote copies, remote signals or barrier semaphores. Data moves between devices by JAX's collectives and lax.ppermute only.
A program may use at most 64 MiB of HBM per device.

```python
import math
import jax
import jax.numpy as jnp
import numpy as np
from jax import lax

TRIPLETS = 2304
IFGS = 1200
DATES = 250
P_DEV = 1536
PIXELS = 12288
N_IFG = 4


def network(key):
    extra = IFGS - (4 * DATES - 10)
    starts = lax.broadcasted_iota(jnp.int32, (DATES, 5), 0)
    spans = lax.broadcasted_iota(jnp.int32, (DATES, 5), 1) + 1
    candidates = DATES - 5
    longer = jax.random.randint(jax.random.fold_in(key, 21), (candidates,), 0, 1 << 16, dtype=jnp.int32)
    longer = longer * candidates + lax.broadcasted_iota(jnp.int32, (candidates,), 0)
    _, picked = lax.top_k(longer, extra)
    marks = jnp.sum((lax.broadcasted_iota(jnp.int32, (DATES, extra), 0) == picked[None, :]).astype(jnp.int32), axis=1)
    inside = (starts + spans <= DATES - 1).astype(jnp.int32)
    exists = jnp.where(spans <= 4, inside, marks[:, None] * inside).astype(jnp.int32)
    flat = exists.reshape(-1)
    places = lax.broadcasted_iota(jnp.int32, (DATES * 5,), 0)
    order = jnp.argsort(jnp.where(flat == 1, places, (1 << 20) + places), stable=True)[:IFGS].astype(jnp.int32)
    first = order // 5
    second = first + order % 5 + 1
    pairs = jnp.stack([first, second], axis=1).astype(jnp.int32)
    rank = (jnp.cumsum(flat) - 1).astype(jnp.int32).reshape(DATES, 5)
    combos = [(p, q) for p in range(1, 5) for q in range(1, 5) if p + q <= 5]
    left = jnp.array(np.array([c[0] for c in combos], dtype=np.int32))
    right = jnp.array(np.array([c[1] for c in combos], dtype=np.int32))
    count = len(combos)
    anchor = lax.broadcasted_iota(jnp.int32, (DATES, count), 0)
    short_a = jnp.broadcast_to(left[None, :], (DATES, count))
    short_b = jnp.broadcast_to(right[None, :], (DATES, count))
    middle = jnp.minimum(anchor + short_a, DATES - 1)
    valid = exists[anchor, short_a - 1] * exists[middle, short_b - 1] * exists[anchor, short_a + short_b - 1]
    total = DATES * count
    noise = jax.random.randint(jax.random.fold_in(key, 22), (total,), 0, 1 << 10, dtype=jnp.int32)
    scores = valid.reshape(-1) * (1 << 24) + noise * total + lax.broadcasted_iota(jnp.int32, (total,), 0)
    _, chosen = lax.top_k(scores, TRIPLETS)
    chosen = chosen.astype(jnp.int32)
    row_a = chosen // count
    which = chosen % count
    span_a = left[which]
    span_b = right[which]
    row_mid = jnp.minimum(row_a + span_a, DATES - 1)
    col_one = rank[row_a, span_a - 1]
    col_two = rank[row_mid, span_b - 1]
    col_long = rank[row_a, span_a + span_b - 1]
    columns = lax.broadcasted_iota(jnp.int32, (TRIPLETS, IFGS), 1)
    signed = (columns == col_one[:, None]).astype(jnp.int32) + (columns == col_two[:, None]).astype(jnp.int32) - (columns == col_long[:, None]).astype(jnp.int32)
    return (signed.astype(jnp.int32), pairs)


def draw_incidence(key, part):
    signed, _ = network(jax.random.fold_in(key, 5))
    return signed


def draw_date_pairs(key, part):
    _, pairs = network(jax.random.fold_in(key, 5))
    return pairs


def draw_phase(key, part):
    block_width = max(P_DEV // 2, 1)
    block_count = PIXELS // block_width
    block_of = (lax.broadcasted_iota(jnp.int32, (PIXELS,), 0) // block_width).astype(jnp.int32)
    inner = jax.random.fold_in(key, 31)
    level_key = jax.random.fold_in(key, 32)
    overall_key = jax.random.fold_in(key, 33)
    rough_key = jax.random.fold_in(key, 34)
    rough = jax.random.uniform(rough_key, (1, PIXELS), jnp.float32, 0.7, 1.4)
    levels = jax.random.uniform(level_key, (block_count,), jnp.float32, -1.0, 0.6)
    overall = 0.25 * jnp.exp(jax.random.uniform(overall_key, (), jnp.float32, -0.5, 0.5))
    spread = overall * jnp.power(10.0, jnp.take(levels, block_of))[None, :] * rough
    values = jnp.clip(jax.random.normal(inner, (IFGS, PIXELS), jnp.float32), -3.0, 3.0) * spread
    return values.astype(jnp.bfloat16)


def shard_levels(own_key, dims, shards, least, top_value):
    def one(dim, blocks):
        steps = jax.random.uniform(jax.random.fold_in(jax.random.fold_in(own_key, 6), dim), (blocks,), jnp.float32, least / len(shards), top_value / len(shards))
        return jnp.repeat(jnp.exp(steps), dims[dim] // blocks).reshape((-1,) + (1,) * (len(dims) - dim - 1))

    level = one(*shards[0])
    for cut in shards[1:]:
        level = level * one(*cut)
    return level


def setup_inputs(seed: int = 0) -> dict:
    seeds = jax.random.split(jax.random.key(seed), 5)
    return {
        "phase": draw_phase(jax.random.fold_in(seeds[4], 71), 0),
        "incidence": draw_incidence(jax.random.fold_in(seeds[4], 71), 0),
        "triplet_weight": jnp.clip(jnp.exp(math.log(3.0) - 2.3025851 * jax.random.uniform(seeds[2], (TRIPLETS,), jnp.float32) ** shard_levels(seeds[2], (TRIPLETS,), ((0, 4),), -0.2, 0.2)), 0.3, 3.0),
        "date_pairs": draw_date_pairs(jax.random.fold_in(seeds[4], 71), 0),
    }


def reference(phase, incidence, triplet_weight, date_pairs):
    signed = incidence.astype(jnp.bfloat16)
    closure = jnp.dot(signed, phase, preferred_element_type=jnp.float32)
    residual = jnp.sin(closure)
    wrapped = residual.astype(jnp.bfloat16)
    misfit = jnp.sum(triplet_weight[:, None] * (1.0 - jnp.cos(closure)), axis=0)
    score = misfit / jnp.sum(triplet_weight)
    relative = score / (jnp.sum(score) / PIXELS)
    blocks = N_IFG
    rows = TRIPLETS // blocks
    signed_blocks = signed.reshape(blocks, rows, IFGS)
    wrapped_blocks = wrapped.reshape(blocks, rows, PIXELS)

    def accumulate(carry, pair):
        part = lax.dot_general(pair[0], pair[1], (((0,), (0,)), ((), ())), preferred_element_type=jnp.float32)
        return carry + part.astype(jnp.bfloat16).astype(jnp.float32), None

    correction, _ = lax.scan(accumulate, jnp.zeros((IFGS, PIXELS), jnp.float32), (signed_blocks, wrapped_blocks))
    span = (date_pairs[:, 1] - date_pairs[:, 0]).astype(jnp.float32)
    corrected = phase.astype(jnp.float32) - correction / (2.0 + span)[:, None]
    return residual, relative, corrected
```

```python
import functools
import math

import jax
import jax.numpy as jnp
from jax import lax
from jax.experimental import pallas as pl
from jax.experimental.pallas import tpu as pltpu
from jax.sharding import PartitionSpec as P


LANES = 128
HALO = 32
NONE = -1.0e6

TURN = 2.0 * math.pi
TURN_HI = 6.28125
TURN_LO = TURN - TURN_HI
HALF_SIN = (0.49999998828912434, -0.02083330953386605, 0.00026040311546377004, -1.5469445175061011e-06, 5.059516426000118e-09)
HALF_COS = (0.9999999534435418, -0.12499976327387889, 0.0026039739862581505, -2.1646402185634008e-05, 9.044442032050874e-08)
SIN = (0.10132113987062294, -0.006620762599308367, 0.00017342015803113834, -2.4978209745388113e-06, 2.029969572939537e-08)


def up(value, step):
    return -(-value // step) * step


def horner(u, coefficients):
    total = jnp.full_like(u, coefficients[-1])
    for c in coefficients[-2::-1]:
        total = total * u + c
    return total


def reduced(x):
    k = jnp.round(x * (1.0 / TURN))
    return (x - k * TURN_HI) - k * TURN_LO


def sine(x):
    r = reduced(x)
    u = r * r
    return (r * (math.pi * math.pi - u)) * horner(u, SIN)


def sine_and_loss(x):
    r = reduced(x)
    u = r * r
    s = r * horner(u, HALF_SIN)
    s2 = s + s
    return s2 * horner(u, HALF_COS), s2 * s


def iota(shape, dim):
    return lax.broadcasted_iota(jnp.int32, shape, dim).astype(jnp.float32)


def index_kernel(n, rows, padded, inc_ref, weight_ref, pay_ref, signed_ref, cols):
    step, steps = pl.program_id(0), pl.num_programs(0)
    me = lax.axis_index("ifg")
    tile = inc_ref.shape[0]
    value = inc_ref[...]
    lane = iota(value.shape, 1)
    one = jnp.min(jnp.where(value > 0, lane, -NONE), axis=1, keepdims=True)
    two = jnp.max(jnp.where(value > 0, lane, NONE), axis=1, keepdims=True)
    long = jnp.max(jnp.where(value < 0, lane, NONE), axis=1, keepdims=True)
    width = signed_ref.shape[1]
    place = iota((tile, width), 1)
    spots = []
    for c in (one, two, long):
        block = jnp.floor((c + 0.5) * (1.0 / rows))
        spot = jnp.zeros_like(c)
        for j in range(n):
            at = jnp.bitwise_xor(me, j).astype(jnp.float32)
            spot = spot + jnp.where(block == at, c - block * rows + j * padded, 0.0)
        spots.append(spot)
    plus = jnp.where((place == spots[0]) | (place == spots[1]), 1.0, 0.0)
    signed_ref[...] = jnp.where(place == spots[2], -1.0, plus).astype(jnp.bfloat16)
    lanes = iota((tile, LANES), 1)
    packed = jnp.where(lanes == 0.0, one, jnp.where(lanes == 1.0, long, jnp.where(lanes == 2.0, two, 0.0)))
    cols[pl.ds(pl.multiple_of(step * tile, tile), tile), :] = packed

    @pl.when(step == steps - 1)
    def _():
        count = cols.shape[0]
        full = pay_ref.shape[1]
        table = jnp.transpose(cols[...])[:8, :]
        row = iota((8, count), 0)
        table = jnp.where(row == 3.0, weight_ref[...], table)
        pay_ref[...] = jnp.where(iota((8, full), 0) < 3.0, NONE, 0.0)
        pay_ref[:, :count] = table


def owner_kernel(n, rows, padded, slots, *refs):
    pays = refs[:n]
    own_ref, before_ref, after_ref, dates_ref, corrected_ref, score_ref, fit, fit_t, weights, scale, total, window, wrapped = refs[n:]
    window_rows = window.shape[0]
    full = pays[0].shape[1]

    @pl.when(pl.program_id(0) == 0)
    def _():
        base = (lax.axis_index("ifg") * rows).astype(jnp.float32)
        lower = iota((full, full), 0)
        upper = iota((full, full), 1)
        ones = jnp.where(lower <= upper, 1.0, 0.0).astype(jnp.bfloat16)
        count = jnp.zeros((1, 1), jnp.float32)
        weight_sum = jnp.zeros((1, 1), jnp.float32)
        table = jnp.zeros((slots, LANES), jnp.float32)
        slot = iota((slots, full), 0)
        for pay in pays:
            here, places = [], []
            for k in range(3):
                d = pay[k : k + 1, :] - base
                inside = (d >= 0.0) & (d < float(rows))
                here.append(inside)
                past = jnp.where(d < 0.0, d + float(padded + HALO), d + float(padded + HALO - rows))
                places.append(jnp.where(inside, d, past) + 1.0)
            touching = jnp.where(here[0] | here[1] | here[2], 1.0, 0.0)
            weight = pay[3:4, :]
            weight_sum = weight_sum + jnp.sum(weight, axis=1, keepdims=True)
            owned = jnp.where(here[0], weight, 0.0)
            mark = jnp.broadcast_to(touching, (16, full)).astype(jnp.bfloat16)
            upto = jnp.dot(mark, ones, preferred_element_type=jnp.float32)[0:1, :]
            rank = jnp.where(touching > 0.0, upto - 1.0 + count, -1.0)
            count = count + jnp.sum(touching, axis=1, keepdims=True)
            parts = []
            for place in places:
                high = jnp.floor(place * (1.0 / 32.0))
                parts += [high, place - 32.0 * high]
            for _ in range(3):
                part = owned.astype(jnp.bfloat16).astype(jnp.float32)
                owned = owned - part
                parts.append(part)
            data = jnp.concatenate(parts + [jnp.zeros((LANES - len(parts), full), jnp.float32)], axis=0)
            data = jnp.where(touching > 0.0, data, 0.0).astype(jnp.bfloat16)
            pick = jnp.where(slot == rank, 1.0, 0.0).astype(jnp.bfloat16)
            table = table + lax.dot_general(pick, data, (((1,), (1,)), ((), ())), preferred_element_type=jnp.float32)
        total[...] = jnp.broadcast_to(weight_sum, total.shape)
        weights[...] = jnp.broadcast_to(table[:, 6:7] + table[:, 7:8] + table[:, 8:9], weights.shape)
        spot = iota((slots, window_rows), 1) + 1.0
        at = [table[:, 2 * k : 2 * k + 1] * 32.0 + table[:, 2 * k + 1 : 2 * k + 2] for k in range(3)]
        plus = jnp.where((spot == at[0]) | (spot == at[2]), 1.0, 0.0)
        fit[...] = jnp.where(spot == at[1], -1.0, plus).astype(jnp.bfloat16)
        across = jnp.transpose(table)
        at = [across[2 * k : 2 * k + 1, :] * 32.0 + across[2 * k + 1 : 2 * k + 2, :] for k in range(3)]
        spot = iota((padded, slots), 0) + 1.0
        plus = jnp.where((spot == at[0]) | (spot == at[2]), 1.0, 0.0)
        fit_t[...] = jnp.where(spot == at[1], -1.0, plus).astype(jnp.bfloat16)
        dates = dates_ref[...].astype(jnp.float32)
        span = dates[1:2, :] - dates[0:1, :]
        wide = up(rows, LANES)
        span = jnp.concatenate([span, jnp.zeros((1, wide - rows), jnp.float32)], axis=1) if wide > rows else span
        column = jnp.transpose(jnp.broadcast_to(span, (LANES, wide)))
        scale[...] = 1.0 / (2.0 + column[: scale.shape[0], :])
        window[...] = jnp.zeros_like(window)

    window[0:rows, :] = own_ref[...]
    window[padded : padded + HALO, :] = before_ref[...]
    window[padded + HALO : padded + 2 * HALO, :] = after_ref[...]
    near = window[...]
    width = near.shape[1]
    tile = LANES
    misfit = jnp.zeros((1, width), jnp.float32)
    for t in range(slots // tile):
        rows_here = slice(t * tile, (t + 1) * tile)
        closure = jnp.dot(fit[rows_here, :], near, preferred_element_type=jnp.float32)
        s, loss = sine_and_loss(closure)
        wrapped[rows_here, :] = s.astype(jnp.bfloat16)
        weight = jnp.concatenate([weights[rows_here, :]] * (width // LANES), axis=1)
        misfit = misfit + jnp.sum(loss * weight, axis=0, keepdims=True)
    score_ref[...] = misfit / total[0:1, 0:1]
    correction = jnp.dot(fit_t[...], wrapped[...], preferred_element_type=jnp.float32)[:rows, :]
    factor = jnp.concatenate([scale[:rows, :]] * (width // LANES), axis=1)
    corrected_ref[...] = own_ref[...].astype(jnp.float32) - correction * factor


def residual_kernel(n, rows, padded, aliased, signed_ref, *refs):
    blocks = refs[:n]
    out_ref, stack = refs[n + aliased :]

    @pl.when(pl.program_id(0) == 0)
    def _():
        stack[...] = jnp.zeros_like(stack)

    for j in range(n):
        stack[j * padded : j * padded + rows, :] = blocks[j][...]
    held = stack[...]
    tile = math.gcd(out_ref.shape[0], 192)
    for t in range(out_ref.shape[0] // tile):
        part = slice(t * tile, (t + 1) * tile)
        closure = jnp.dot(signed_ref[part, :], held, preferred_element_type=jnp.float32)
        out_ref[part, :] = sine(closure)


def gathered(block, bits, exchange):
    held = {0: block}
    for bit in bits:
        held.update({mask ^ bit: exchange(value, bit) for mask, value in list(held.items())})
    return held


def local(n_pix, phase, incidence, triplet_weight, date_pairs):
    n = lax.axis_size("ifg")
    rows, pixels = phase.shape
    triplets, ifgs = incidence.shape
    padded = up(rows, 16)
    full = up(triplets, LANES)
    assert n & (n - 1) == 0 and rows >= HALO and pixels % (4 * LANES) == 0
    f32, bf16 = jnp.float32, jnp.bfloat16

    def exchange(value, mask):
        return lax.ppermute(value, "ifg", [(i, i ^ mask) for i in range(n)])

    half = pixels // 2
    bits = [1 << b for b in range(n.bit_length() - 1)]
    left = gathered(phase[:, :half], bits, exchange)
    right = gathered(phase[:, half:], bits[::-1], exchange)
    before = lax.ppermute(phase[rows - HALO :, :], "ifg", [(i, i + 1) for i in range(n - 1)])
    after = lax.ppermute(phase[:HALO, :], "ifg", [(i + 1, i) for i in range(n - 1)])

    tile = math.gcd(triplets, 144)
    stacked = n * padded
    pay, signed = pl.pallas_call(
        functools.partial(index_kernel, n, rows, padded),
        grid=(triplets // tile,),
        in_specs=[pl.BlockSpec((tile, ifgs), lambda i: (i, 0)), pl.BlockSpec((1, triplets), lambda i: (0, 0))],
        out_specs=[pl.BlockSpec((8, full), lambda i: (0, 0)), pl.BlockSpec((tile, stacked), lambda i: (i, 0))],
        out_shape=[jax.ShapeDtypeStruct((8, full), f32), jax.ShapeDtypeStruct((triplets, stacked), bf16)],
        scratch_shapes=[pltpu.VMEM((triplets, LANES), f32)],
        cost_estimate=pl.CostEstimate(flops=10**7, bytes_accessed=4 * triplets * ifgs, transcendentals=0),
        name="index",
    )(incidence, triplet_weight.reshape(1, triplets))

    pays = [pay] + [exchange(pay, mask) for mask in range(1, n)]

    slots = min(up(2 * rows + 37, LANES), n * full)
    width = pixels // 4
    corrected, score = pl.pallas_call(
        functools.partial(owner_kernel, n, rows, padded, slots),
        grid=(pixels // width,),
        in_specs=[pl.BlockSpec((8, full), lambda i: (0, 0))] * n
        + [
            pl.BlockSpec((rows, width), lambda i: (0, i)),
            pl.BlockSpec((HALO, width), lambda i: (0, i)),
            pl.BlockSpec((HALO, width), lambda i: (0, i)),
            pl.BlockSpec((2, rows), lambda i: (0, 0)),
        ],
        out_specs=[pl.BlockSpec((rows, width), lambda i: (0, i)), pl.BlockSpec((1, width), lambda i: (0, i))],
        out_shape=[jax.ShapeDtypeStruct((rows, pixels), f32), jax.ShapeDtypeStruct((1, pixels), f32)],
        scratch_shapes=[
            pltpu.VMEM((slots, padded + 2 * HALO), bf16),
            pltpu.VMEM((padded, slots), bf16),
            pltpu.VMEM((slots, LANES), f32),
            pltpu.VMEM((padded, LANES), f32),
            pltpu.VMEM((8, LANES), f32),
            pltpu.VMEM((padded + 2 * HALO, width), bf16),
            pltpu.VMEM((slots, width), bf16),
        ],
        cost_estimate=pl.CostEstimate(flops=4 * slots * rows * pixels, bytes_accessed=6 * rows * pixels, transcendentals=0),
        name="owner",
    )(*pays, phase, before, after, date_pairs.T)

    score = score + sum(exchange(score, mask) for mask in range(1, n))
    mean_score = lax.psum(jnp.sum(score), "pix") / (pixels * n_pix)
    relative = (score / mean_score).reshape(pixels)

    def residuals(held, start, into):
        width = half // 2
        first = start // width
        aliased = into is not None
        blocks = [pl.BlockSpec((rows, width), lambda i: (0, i + first))]
        blocks += [pl.BlockSpec((rows, width), lambda i: (0, i))] * (n - 1)
        values = [phase] + [held[mask] for mask in range(1, n)]
        if aliased:
            blocks.append(pl.BlockSpec(memory_space=pl.ANY))
            values.append(into)
        return pl.pallas_call(
            functools.partial(residual_kernel, n, rows, padded, int(aliased)),
            grid=(half // width,),
            in_specs=[pl.BlockSpec((triplets, stacked), lambda i: (0, 0))] + blocks,
            out_specs=pl.BlockSpec((triplets, width), lambda i: (0, i + first)),
            out_shape=jax.ShapeDtypeStruct((triplets, pixels), f32),
            scratch_shapes=[pltpu.VMEM((stacked, width), bf16)],
            input_output_aliases={n + 1: 0} if aliased else {},
            cost_estimate=pl.CostEstimate(flops=2 * triplets * stacked * half, bytes_accessed=4 * triplets * half, transcendentals=0),
            name="residual",
        )(signed, *values)

    residual = residuals(left, 0, None)
    residual = residuals(right, half, residual)
    return residual, relative, corrected


def solution(mesh):
    return jax.shard_map(
        functools.partial(local, mesh.shape["pix"]),
        mesh=mesh,
        in_specs=(P("ifg", "pix"), P("ifg", None), P("ifg"), P("ifg", None)),
        out_specs=(P("ifg", "pix"), P("pix"), P("ifg", "pix")),
        check_vma=False,
    )
```
